128 devices in a mesh: seq: 32 (over x, y, core), head: 4 (over z).
Axes of the slice: x: 4, y: 4, z: 4, core: 2. Of those that a mesh axis runs over, the one named last changes fastest.
Arguments:
- queries: bfloat16 [8192, 4096], P('seq', 'head'), may hold values from -7.1875 to 7.1875
- keys: bfloat16 [8192, 1024], P(('seq', 'head')), may hold values from -7.1875 to 7.1875
- values: bfloat16 [8192, 1024], P(('seq', 'head')), may hold values from -6 to 6
- outputs: bfloat16 [8192, 4096], P('seq', 'head'), may hold values from -1.1953125 to 1.1953125
- out_grad: bfloat16 [8192, 4096], P('seq', 'head'), may hold values from -6 to 6
- log_norm: float32 [32, 8192], P('head', 'seq'), as said below
- block_order: int32 [64], replicated, may hold values from 0 to 63, as said below
Outputs:
- query_grad: bfloat16 [8192, 4096], P('seq', 'head')
- key_gradient_rows: bfloat16 [8192, 1024], P(('seq', 'head'))
- value_gradient_rows: bfloat16 [8192, 1024], P(('seq', 'head'))
The draws below stay inside these ranges and needn't reach their ends.
Inputs may be any that keep to these rules, and one draw needn't show every extreme that they name: `block_order`: A permutation of 0 to 63. log_norm[h, i] lies within 0.6 of one plus the natural logarithm of 1 + pos[i].
All inputs are finite; a program needn't handle non-finite values.
Results may differ from the reference program's by a relative error of at most 0.014.
Values may be sent and summed in bfloat16 or wider, within the bound.
A program may use at most 192 MiB of HBM per device.

```python
import jax
import jax.numpy as jnp
from jax import lax

QUERY_HEADS = 32
KEY_VALUE_HEADS = 8
HEAD_SIZE = 128
TOK_DEV = 256
SEQUENCE_TOKENS = 8192
N_SEQ = 32


def order_helper(key):
    return jax.random.permutation(jax.random.fold_in(key, 7), 2 * N_SEQ).astype(jnp.int32)


def draw_block_order(key, part):
    return order_helper(key)


def draw_log_norm(key, part):
    order = order_helper(key)
    half = TOK_DEV // 2
    rows = jnp.arange(SEQUENCE_TOKENS, dtype=jnp.int32)
    pos = (order[rows // half] * half + rows % half).astype(jnp.float32)
    base = jnp.log(1.0 + pos)[None, :] + 1.0
    noise = jax.random.uniform(jax.random.fold_in(key, 11), (QUERY_HEADS, SEQUENCE_TOKENS), jnp.float32, -0.3, 0.3)
    return (base + noise).astype(jnp.float32)


def block_levels(rng, shape, shards, smallest, top_value):
    level = 1.0
    for position, parts in shards:
        heights = jax.random.uniform(jax.random.fold_in(jax.random.fold_in(rng, 6), position), (parts,), jnp.float32, smallest / len(shards), top_value / len(shards))
        level = level * jnp.repeat(jnp.exp(heights), shape[position] // parts).reshape((-1,) + (1,) * (len(shape) - 1 - position))
    return level


def gaussian(key, extent, width, most, pieces=(), kind=jnp.bfloat16):
    entries = jax.random.normal(key, extent, jnp.float32) * width
    if len(pieces) > 0:
        entries = block_levels(key, extent, pieces, -0.22, 0.18) * entries
    return jnp.clip(entries, min=-most, max=most).astype(kind)


def setup_inputs(seed: int = 0) -> dict:
    streams_of = jax.random.split(jax.random.key(seed), 8)
    queries = gaussian(streams_of[0], (SEQUENCE_TOKENS, QUERY_HEADS * HEAD_SIZE), 1.2, 7.1875, ((0, 32), (1, 4)))
    keys = gaussian(streams_of[1], (SEQUENCE_TOKENS, KEY_VALUE_HEADS * HEAD_SIZE), 1.2, 7.1875, ((0, 128),))
    values = gaussian(streams_of[2], (SEQUENCE_TOKENS, KEY_VALUE_HEADS * HEAD_SIZE), 1.0, 6.0, ((0, 128),))
    outputs = gaussian(streams_of[3], (SEQUENCE_TOKENS, QUERY_HEADS * HEAD_SIZE), 0.2, 1.1953125, ((0, 32), (1, 4)))
    out_grad = gaussian(streams_of[4], (SEQUENCE_TOKENS, QUERY_HEADS * HEAD_SIZE), 1.0, 6.0, ((0, 32), (1, 4)))
    log_norm = draw_log_norm(jax.random.fold_in(streams_of[7], 71), 0)
    block_order = draw_block_order(jax.random.fold_in(streams_of[7], 71), 0)
    return {"queries": queries, "keys": keys, "values": values, "outputs": outputs, "out_grad": out_grad, "log_norm": log_norm, "block_order": block_order}


def token_positions(block_order):
    half = TOK_DEV // 2
    rows = jnp.arange(SEQUENCE_TOKENS, dtype=jnp.int32)
    return (block_order[rows // half] * half + rows % half).astype(jnp.int32)


def reference(queries, keys, values, outputs, out_grad, log_norm, block_order):
    scale = HEAD_SIZE ** -0.5
    group_ratio = QUERY_HEADS // KEY_VALUE_HEADS
    pos = token_positions(block_order)
    delta = jnp.sum((out_grad.astype(jnp.float32) * outputs.astype(jnp.float32)).reshape(SEQUENCE_TOKENS, QUERY_HEADS, HEAD_SIZE), -1)
    qblock = 512 if SEQUENCE_TOKENS % 512 == 0 else SEQUENCE_TOKENS
    nblocks = SEQUENCE_TOKENS // qblock

    def queries_per_group(g):
        kg = lax.dynamic_slice_in_dim(keys, g * HEAD_SIZE, HEAD_SIZE, 1).astype(jnp.float32)
        vg = lax.dynamic_slice_in_dim(values, g * HEAD_SIZE, HEAD_SIZE, 1).astype(jnp.float32)
        qg = lax.dynamic_slice_in_dim(queries, g * group_ratio * HEAD_SIZE, group_ratio * HEAD_SIZE, 1).reshape(SEQUENCE_TOKENS, group_ratio, HEAD_SIZE)
        dg = lax.dynamic_slice_in_dim(out_grad, g * group_ratio * HEAD_SIZE, group_ratio * HEAD_SIZE, 1).reshape(SEQUENCE_TOKENS, group_ratio, HEAD_SIZE)
        lg = lax.dynamic_slice_in_dim(log_norm, g * group_ratio, group_ratio, 0)
        eg = lax.dynamic_slice_in_dim(delta, g * group_ratio, group_ratio, 1)

        def step(carry, b):
            keys_gradient, values_gradient = carry
            start = (b * qblock).astype(jnp.int32)
            qb = lax.dynamic_slice_in_dim(qg, start, qblock, 0).astype(jnp.float32)
            db = lax.dynamic_slice_in_dim(dg, start, qblock, 0).astype(jnp.float32)
            lb = lax.dynamic_slice_in_dim(lg, start, qblock, 1)
            eb = lax.dynamic_slice_in_dim(eg, start, qblock, 0)
            qpos = lax.dynamic_slice_in_dim(pos, start, qblock, 0)
            scores = jnp.einsum("trd,nd->rtn", qb, kg) * scale
            visible = pos[None, :] <= qpos[:, None]
            prob = jnp.where(visible[None], jnp.exp(scores - lb[:, :, None]), 0.0)
            dprob = jnp.einsum("trd,nd->rtn", db, vg)
            dscore = prob * (dprob - eb.T[:, :, None])
            prob_low = prob.astype(jnp.bfloat16).astype(jnp.float32)
            dscore_low = dscore.astype(jnp.bfloat16).astype(jnp.float32)
            values_gradient = values_gradient + jnp.einsum("rtn,trd->nd", prob_low, db)
            keys_gradient = keys_gradient + scale * jnp.einsum("rtn,trd->nd", dscore_low, qb)
            queries_gradient = scale * jnp.einsum("rtn,nd->trd", dscore_low, kg)
            return (keys_gradient, values_gradient), queries_gradient.astype(jnp.bfloat16)

        zeros = jnp.zeros((SEQUENCE_TOKENS, HEAD_SIZE), jnp.float32)
        (keys_gradient, values_gradient), queries_gradient = lax.scan(step, (zeros, zeros), jnp.arange(nblocks, dtype=jnp.int32))
        return queries_gradient.reshape(SEQUENCE_TOKENS, group_ratio * HEAD_SIZE), keys_gradient.astype(jnp.bfloat16), values_gradient.astype(jnp.bfloat16)

    queries_gradient, keys_gradient, values_gradient = lax.map(queries_per_group, jnp.arange(KEY_VALUE_HEADS, dtype=jnp.int32))
    query_grad = jnp.transpose(queries_gradient, (1, 0, 2)).reshape(SEQUENCE_TOKENS, QUERY_HEADS * HEAD_SIZE)
    key_gradient_rows = jnp.transpose(keys_gradient, (1, 0, 2)).reshape(SEQUENCE_TOKENS, KEY_VALUE_HEADS * HEAD_SIZE)
    value_gradient_rows = jnp.transpose(values_gradient, (1, 0, 2)).reshape(SEQUENCE_TOKENS, KEY_VALUE_HEADS * HEAD_SIZE)
    return (query_grad, key_gradient_rows, value_gradient_rows)
```

```python
import functools

import jax
import jax.numpy as jnp
from jax import lax
from jax.experimental import pallas as pl
from jax.experimental.pallas import tpu as pltpu
from jax.sharding import PartitionSpec as P

HEAD_SIZE = 128
RATIO = 4
SCALE = HEAD_SIZE ** (-0.5)
LOG2E = 1.4426950408889634
BIG = 131072.0
MESH = pl.DeviceIdType.MESH
BF = jnp.bfloat16
F32 = jnp.float32


def ring_order(i):
    return i + (i // 2) * (1 - 2 * (i % 2))


def chunk_of(t):
    j = t - 4
    near = jnp.where(t < 4, ring_order(t), ring_order(jnp.where(t < 12, j // 2, t - 12)))
    e = jnp.where(t < 4, 0, jnp.where(t < 12, 1 + 2 * (j % 2), 2))
    return near, e


def kernel(
    nz,
    q_ref, k_ref, v_ref, o_ref, do_ref, lse_ref, ktab_ref, qtab_ref,
    dq_ref, dk_ref, dv_ref,
    kv, sq, sdo, so, slse, qa, doa, qt, dot_, ktail, pbig, dsbig, dqacc,
    pbuf, r1, s2, r2, fin, dqs,
    s0s, s0r, sbs, sbr, axs, axr, ays, ayr, rks, rkr, rvs, rvr,
    r1s, r1r, r2s, r2r, s4s, s4r, dqss, dqsr,
):
    s = lax.axis_index("seq")
    z = lax.axis_index("head")
    x, y, c = s // 8, (s // 2) % 4, s % 2
    rows = q_ref.shape[0]
    piece = k_ref.shape[0]
    chip = 2 * rows
    blk = rows // 2
    half = RATIO * HEAD_SIZE
    nm = 2 * nz

    def dev(xx, yy, cc):
        return ((xx % 4) * 4 + (yy % 4)) * 2 + cc

    me = c * nz + z

    def member(r):
        m = (me + r) % nm
        return m // nz, m % nz

    barrier = pltpu.get_barrier_semaphore()
    for r in range(1, nm):
        cc, zz = member(r)
        pl.semaphore_signal(barrier, inc=1, device_id=(dev(x, y, cc), zz), device_id_type=MESH)
    for d in (1, 2, 3):
        pl.semaphore_signal(barrier, inc=1, device_id=(dev(x + d, y, c), z), device_id_type=MESH)
        pl.semaphore_signal(barrier, inc=1, device_id=(dev(x, y + d, c), z), device_id_type=MESH)
    pl.semaphore_wait(barrier, nm - 1 + 6)

    def rcopy(src, dst, ss, rs, to):
        return pltpu.make_async_remote_copy(
            src_ref=src, dst_ref=dst, send_sem=ss, recv_sem=rs,
            device_id=to, device_id_type=MESH)

    def s0_copy(r, w):
        cc, zz = member(r)
        g = pl.multiple_of((2 * zz + cc) * HEAD_SIZE, HEAD_SIZE)
        src = (k_ref, v_ref)[w].at[:, pl.ds(g, HEAD_SIZE)]
        off = pl.multiple_of(c * rows + z * piece, piece)
        return rcopy(src, kv.at[x, y, w, pl.ds(off, piece), :],
                     s0s.at[r, w], s0r.at[r, w], (dev(x, y, cc), zz))

    for r in range(1, nm):
        for w in range(2):
            s0_copy(r, w).start()

    other = pl.multiple_of((1 - c) * half, half)
    mine = pl.multiple_of(c * half, half)
    sib = (dev(x, y, 1 - c), z)
    sib_copies = [
        rcopy(q_ref.at[:, pl.ds(other, half)], sq, sbs.at[0], sbr.at[0], sib),
        rcopy(do_ref.at[:, pl.ds(other, half)], sdo, sbs.at[1], sbr.at[1], sib),
        rcopy(o_ref.at[:, pl.ds(other, half)], so, sbs.at[2], sbr.at[2], sib),
        rcopy(lse_ref, slse, sbs.at[3], sbr.at[3], sib),
    ]
    for cp in sib_copies:
        cp.start()

    own_off = pl.multiple_of(c * rows + z * piece, piece)
    own_g = pl.multiple_of((2 * z + c) * HEAD_SIZE, HEAD_SIZE)
    kv[x, y, 0, pl.ds(own_off, piece), :] = k_ref[:, pl.ds(own_g, HEAD_SIZE)]
    kv[x, y, 1, pl.ds(own_off, piece), :] = v_ref[:, pl.ds(own_g, HEAD_SIZE)]

    lane = lax.broadcasted_iota(jnp.int32, (blk, HEAD_SIZE), 1)

    def three(col, rest):
        hi = col.astype(BF).astype(F32)
        mid = (col - hi).astype(BF).astype(F32)
        lo = col - hi - mid
        return jnp.where(lane == 0, hi, jnp.where(lane == 1, mid, jnp.where(lane == 2, lo, rest))).astype(BF)

    chip_block = (x * 4 + y) * 4

    def prepare(qr, dor, orf, lr, col0, core):
        for b in range(2):
            rs = pl.ds(b * blk, blk)
            dst = pl.ds(pl.multiple_of(core * rows + b * blk, blk), blk)
            therm = jnp.broadcast_to(qtab_ref[pl.ds(chip_block + 2 * core + b, 1), :], (blk, HEAD_SIZE))
            zero = jnp.zeros((blk, HEAD_SIZE), F32)
            for h in range(RATIO):
                cols = pl.ds(pl.multiple_of(col0 + h * HEAD_SIZE, HEAD_SIZE), HEAD_SIZE)
                q = qr[rs, cols]
                do = dor[rs, cols]
                lse = jnp.where(c == 0, lr[rs, h:h + 1], lr[rs, RATIO + h:RATIO + h + 1])
                delta = jnp.sum(do.astype(F32) * orf[rs, cols].astype(F32), axis=1, keepdims=True)
                qa[h, dst, 0:HEAD_SIZE] = q
                qa[h, dst, HEAD_SIZE:] = three(lse * (-1.0 / SCALE), therm)
                doa[h, dst, 0:HEAD_SIZE] = do
                doa[h, dst, HEAD_SIZE:] = three(-delta, zero)
                tdst = pl.ds(pl.multiple_of(h * chip + core * rows + b * blk, blk), blk)
                qt[:, tdst] = q.astype(F32).T.astype(BF)
                dot_[:, tdst] = do.astype(F32).T.astype(BF)

    prepare(q_ref, do_ref, o_ref, lse_ref, mine, c)
    dqacc[...] = jnp.zeros_like(dqacc)
    lane_v = lax.broadcasted_iota(jnp.int32, (chip, HEAD_SIZE), 1)
    ones_tail = jnp.where(lane_v < 3, 1.0, 0.0).astype(BF)

    for r in range(1, nm):
        for w in range(2):
            s0_copy(r, w).wait_recv()

    def ax_copy(d):
        return rcopy(kv.at[x, y], kv.at[x, y], axs.at[d], axr.at[d], (dev(x + d, y, c), z))

    def ay_copy(d, e):
        xs = (x - d + 4) % 4
        return rcopy(kv.at[xs, y], kv.at[xs, y], ays.at[d, e], ayr.at[d, e], (dev(x, y + e, c), z))

    def relay_k(d):
        xs, ys = (x - d + 4) % 4, (y + 3) % 4
        return rcopy(kv.at[xs, ys, 0], kv.at[xs, ys, 0], rks.at[d], rkr.at[d], (dev(x, y + 1, c), z))

    def relay_v(d):
        xs, ys = (x - d + 4) % 4, (y + 1) % 4
        return rcopy(kv.at[xs, ys, 1], kv.at[xs, ys, 1], rvs.at[d], rvr.at[d], (dev(x, y + 3, c), z))

    def ax_wait(d):
        xs = (x - d + 4) % 4
        rcopy(kv.at[xs, y], kv.at[xs, y], axs.at[d], axr.at[d], (dev(x + d, y, c), z)).wait_recv()

    def ay_wait(d, e):
        xs, ys = (x - d + 4) % 4, (y - e + 4) % 4
        rcopy(kv.at[xs, ys], kv.at[xs, ys], ays.at[d, e], ayr.at[d, e], (dev(x, y + e, c), z)).wait_recv()

    def far_wait(d):
        xs, ys = (x - d + 4) % 4, (y + 2) % 4
        rcopy(kv.at[xs, ys, 0], kv.at[xs, ys, 0], rks.at[d], rkr.at[d], (dev(x, y + 1, c), z)).wait_recv()
        rcopy(kv.at[xs, ys, 1], kv.at[xs, ys, 1], rvs.at[d], rvr.at[d], (dev(x, y + 3, c), z)).wait_recv()

    for d in (1, 3, 2):
        ax_copy(d).start()
    for e in (1, 3):
        ay_copy(0, e).start()

    for cp in sib_copies:
        cp.wait_recv()
    prepare(sq, sdo, so, slse, 0, 1 - c)

    def compute(d, e, masked):
        xs, ys = (x - d + 4) % 4, (y - e + 4) % 4
        kb = (xs * 4 + ys) * 4
        for b in range(4):
            ktail[b * blk:(b + 1) * blk, :] = jnp.broadcast_to(
                ktab_ref[pl.ds(kb + b, 1), :], (blk, HEAD_SIZE)).astype(BF)
        key = kv[xs, ys, 0]
        ka = jnp.concatenate([key, ktail[...]], axis=1)
        va = jnp.concatenate([kv[xs, ys, 1], ones_tail], axis=1)
        nt = (((1,), (1,)), ((), ()))
        for h in range(RATIO):
            sc = lax.dot_general(qa[h], ka, nt, preferred_element_type=F32)
            dp = lax.dot_general(doa[h], va, nt, preferred_element_type=F32)
            p = jnp.exp2(sc * (SCALE * LOG2E))
            if masked:
                row = lax.broadcasted_iota(jnp.int32, p.shape, 0)
                col = lax.broadcasted_iota(jnp.int32, p.shape, 1)
                p = jnp.where((col > row) & (col // blk == row // blk), 0.0, p)
            ds = (p * dp).astype(BF)
            pbig[h * chip:(h + 1) * chip, :] = p.astype(BF)
            dsbig[h * chip:(h + 1) * chip, :] = ds
            dqacc[h] += jnp.dot(ds, key, preferred_element_type=F32)
        pbuf[d, e, 0] = (jnp.dot(qt[...], dsbig[...], preferred_element_type=F32) * SCALE).astype(BF)
        pbuf[d, e, 1] = jnp.dot(dot_[...], pbig[...], preferred_element_type=F32).astype(BF)

    def r1_copy(d, e):
        return rcopy(pbuf.at[d, e], r1.at[d, e], r1s.at[d, e], r1r.at[d, e], (dev(x - d + 4, y, c), z))

    def r2_copy(e):
        return rcopy(s2.at[e], r2.at[e], r2s.at[e], r2r.at[e], (dev(x, y - e + 4, c), z))

    def sum_x(e, w):
        tot = pbuf[0, e, w].astype(F32)
        for d in (1, 2, 3):
            tot = tot + r1[d, e, w].astype(F32)
        return tot

    def combine(e):
        for d in (1, 2, 3):
            r1_copy(d, e).wait_recv()
        for w in range(2):
            s2[e, w] = sum_x(e, w).astype(BF)

    compute(0, 0, True)

    def step(t, carry):
        d, e = chunk_of(t)

        @pl.when(e == 0)
        def _():
            ax_wait(d)
            ay_copy(d, 1).start()
            ay_copy(d, 3).start()

        @pl.when(e == 1)
        def _():
            ay_wait(d, 1)
            relay_k(d).start()

        @pl.when(e == 3)
        def _():
            ay_wait(d, 3)
            relay_v(d).start()

        @pl.when(e == 2)
        def _():
            far_wait(d)

        pd, pe = chunk_of(t - 1)

        @pl.when(pd != 0)
        def _():
            r1_copy(pd, pe).start()

        @pl.when(t == 15)
        def _():
            r2_copy(1).start()

        compute(d, e, False)

        @pl.when(t == 14)
        def _():
            combine(1)

        @pl.when(t == 15)
        def _():
            combine(3)

        return carry

    lax.fori_loop(1, 16, step, 0)
    r1_copy(2, 2).start()
    r2_copy(3).start()

    orow = pl.multiple_of((1 - c) * rows, rows)
    mrow = pl.multiple_of(c * rows, rows)
    for h in range(RATIO):
        dqs[:, h * HEAD_SIZE:(h + 1) * HEAD_SIZE] = (dqacc[h, pl.ds(orow, rows), :] * SCALE).astype(BF)
    for h in range(RATIO):
        cols = pl.ds(pl.multiple_of(mine + h * HEAD_SIZE, HEAD_SIZE), HEAD_SIZE)
        dq_ref[:, cols] = (dqacc[h, pl.ds(mrow, rows), :] * SCALE).astype(BF)
    dq_copy = rcopy(dqs, dq_ref.at[:, pl.ds(mine, half)], dqss.at[0], dqsr.at[0], sib)
    dq_copy.start()

    combine(2)
    for d in (1, 2, 3):
        r1_copy(d, 0).wait_recv()
    tots = [sum_x(0, w) for w in range(2)]
    r2_copy(2).start()
    for e in (1, 3):
        r2_copy(e).wait_recv()
        tots = [tots[w] + r2[e, w].astype(F32) for w in range(2)]
    r2_copy(2).wait_recv()
    for w in range(2):
        fin[w] = (tots[w] + r2[2, w].astype(F32)).T.astype(BF)

    def s4_copy(r, w):
        cc, zz = member(r)
        off = pl.multiple_of(cc * rows + zz * piece, piece)
        dst = (dk_ref, dv_ref)[w].at[:, pl.ds(own_g, HEAD_SIZE)]
        return rcopy(fin.at[w, pl.ds(off, piece), :], dst, s4s.at[r, w], s4r.at[r, w], (dev(x, y, cc), zz))

    for r in range(1, nm):
        for w in range(2):
            s4_copy(r, w).start()
    dk_ref[:, pl.ds(own_g, HEAD_SIZE)] = fin[0, pl.ds(own_off, piece), :]
    dv_ref[:, pl.ds(own_g, HEAD_SIZE)] = fin[1, pl.ds(own_off, piece), :]

    def s4_wait(r, w):
        m = (me - r + nm) % nm
        cc, zz = m // nz, m % nz
        g = pl.multiple_of((2 * zz + cc) * HEAD_SIZE, HEAD_SIZE)
        dst = (dk_ref, dv_ref)[w].at[:, pl.ds(g, HEAD_SIZE)]
        rcopy(fin.at[w, pl.ds(0, piece), :], dst, s4s.at[r, w], s4r.at[r, w], sib).wait_recv()

    for r in range(1, nm):
        for w in range(2):
            s4_wait(r, w)
    rcopy(dqs, dq_ref.at[:, pl.ds(other, half)], dqss.at[0], dqsr.at[0], sib).wait_recv()

    for r in range(1, nm):
        for w in range(2):
            s0_copy(r, w).wait_send()
            s4_copy(r, w).wait_send()
    for cp in sib_copies:
        cp.wait_send()
    dq_copy.wait_send()
    for d in (1, 2, 3):
        ax_copy(d).wait_send()
    for e in (1, 2, 3):
        r2_copy(e).wait_send()
    for d in range(4):
        ay_copy(d, 1).wait_send()
        ay_copy(d, 3).wait_send()
        relay_k(d).wait_send()
        relay_v(d).wait_send()
        if d:
            for e in range(4):
                r1_copy(d, e).wait_send()


def fused(nz, queries, keys, values, outputs, out_grad, lse, ktab, qtab):
    rows, piece = queries.shape[0], keys.shape[0]
    chip = 2 * rows
    half = RATIO * HEAD_SIZE
    nm = 2 * nz
    dma = pltpu.SemaphoreType.DMA
    vm = pl.BlockSpec(memory_space=pltpu.VMEM)
    return pl.pallas_call(
        functools.partial(kernel, nz),
        out_shape=(
            jax.ShapeDtypeStruct(queries.shape, BF),
            jax.ShapeDtypeStruct(keys.shape, BF),
            jax.ShapeDtypeStruct(values.shape, BF),
        ),
        in_specs=[vm] * 8,
        out_specs=(vm, vm, vm),
        scratch_shapes=[
            pltpu.VMEM((4, 4, 2, chip, HEAD_SIZE), BF),
            pltpu.VMEM((rows, half), BF),
            pltpu.VMEM((rows, half), BF),
            pltpu.VMEM((rows, half), BF),
            pltpu.VMEM(lse.shape, F32),
            pltpu.VMEM((RATIO, chip, 2 * HEAD_SIZE), BF),
            pltpu.VMEM((RATIO, chip, 2 * HEAD_SIZE), BF),
            pltpu.VMEM((HEAD_SIZE, RATIO * chip), BF),
            pltpu.VMEM((HEAD_SIZE, RATIO * chip), BF),
            pltpu.VMEM((chip, HEAD_SIZE), BF),
            pltpu.VMEM((RATIO * chip, chip), BF),
            pltpu.VMEM((RATIO * chip, chip), BF),
            pltpu.VMEM((RATIO, chip, HEAD_SIZE), F32),
            pltpu.VMEM((4, 4, 2, HEAD_SIZE, chip), BF),
            pltpu.VMEM((4, 4, 2, HEAD_SIZE, chip), BF),
            pltpu.VMEM((4, 2, HEAD_SIZE, chip), BF),
            pltpu.VMEM((4, 2, HEAD_SIZE, chip), BF),
            pltpu.VMEM((2, chip, HEAD_SIZE), BF),
            pltpu.VMEM((rows, half), BF),
            dma((nm, 2)), dma((nm, 2)), dma((4,)), dma((4,)),
            dma((4,)), dma((4,)), dma((4, 4)), dma((4, 4)),
            dma((4,)), dma((4,)), dma((4,)), dma((4,)),
            dma((4, 4)), dma((4, 4)), dma((4,)), dma((4,)),
            dma((nm, 2)), dma((nm, 2)), dma((1,)), dma((1,)),
        ],
        compiler_params=pltpu.CompilerParams(
            collective_id=0, has_side_effects=True, vmem_limit_bytes=60 * 1024 * 1024),
    )(queries, keys, values, outputs, out_grad, lse, ktab, qtab)


def local(nz, queries, keys, values, outputs, out_grad, log_norm, block_order):
    blocks = block_order.shape[0]
    lane = jnp.arange(HEAD_SIZE, dtype=jnp.int32)[None, :]
    slot = lane - (HEAD_SIZE - blocks)
    pos = block_order[:, None]
    ktab = jnp.where((lane < 3) | (slot == pos), 1.0, 0.0).astype(F32)
    qtab = jnp.where(slot > pos, -BIG, 0.0).astype(F32)
    return fused(nz, queries, keys, values, outputs, out_grad, log_norm.T, ktab, qtab)


def solution(mesh):
    in_specs = (
        P("seq", "head"),
        P(("seq", "head"), None),
        P(("seq", "head"), None),
        P("seq", "head"),
        P("seq", "head"),
        P("head", "seq"),
        P(),
    )
    out_specs = (P("seq", "head"), P(("seq", "head"), None), P(("seq", "head"), None))
    return jax.shard_map(
        functools.partial(local, mesh.shape["head"]), mesh=mesh,
        in_specs=in_specs, out_specs=out_specs, check_vma=False)
```

```python
import functools

import jax
import jax.numpy as jnp
from jax import lax
from jax.experimental import pallas as pl
from jax.experimental.pallas import tpu as pltpu
from jax.sharding import PartitionSpec as P

HEAD_SIZE = 128
RATIO = 4
SCALE = HEAD_SIZE ** (-0.5)
LOG2E = 1.4426950408889634
BIG = 131072.0
MESH = pl.DeviceIdType.MESH
BF = jnp.bfloat16
F32 = jnp.float32


ORDER = (
    (0, 0), (0, 1), (0, 3), (2, 0), (1, 1), (3, 3), (2, 1), (2, 3),
    (3, 1), (1, 3), (2, 2), (0, 2), (1, 2), (3, 2), (1, 0), (3, 0),
)


def pick(t, values):
    out = values[0]
    for i, v in enumerate(values):
        out = jnp.where(t == i, v, out)
    return out


def kernel(
    nz,
    qh, kh, vh, oh, doh, lseh, boh,
    dq_ref, dk_ref, dv_ref,
    q_ref, k_ref, v_ref, o_ref, do_ref, lse_ref, bo_ref,
    kv, sq, sdo, so, slse, lpad, lt, qa, doa, qt, dot_, ktail, pbig, dsbig, dqacc,
    pbuf, r1, ra, s2, r2, fin, dqs,
    ins, s0s, s0r, sbs, sbr, axs, axr, ays, ayr, fxs, fxr, fys, fyr,
    r1s, r1r, ras, rar, r2s, r2r, s4s, s4r, dqss, dqsr,
):
    s = lax.axis_index("seq")
    z = lax.axis_index("head")
    x, y, c = s // 8, (s // 2) % 4, s % 2
    rows = q_ref.shape[0]
    piece = k_ref.shape[0]
    chip = 2 * rows
    blk = rows // 2
    half = RATIO * HEAD_SIZE
    nm = 2 * nz

    def dev(xx, yy, cc):
        return ((xx % 4) * 4 + (yy % 4)) * 2 + cc

    me = c * nz + z

    def member(r):
        m = (me + r) % nm
        return m // nz, m % nz

    loads = [
        pltpu.make_async_copy(src, dst, ins.at[i])
        for i, (src, dst) in enumerate((
            (kh, k_ref), (vh, v_ref), (qh, q_ref), (doh, do_ref), (oh, o_ref), (lseh, lse_ref), (boh, bo_ref)))
    ]
    for cp in loads:
        cp.start()

    barrier = pltpu.get_barrier_semaphore()
    for r in range(1, nm):
        cc, zz = member(r)
        pl.semaphore_signal(barrier, inc=1, device_id=(dev(x, y, cc), zz), device_id_type=MESH)
    for d in (1, 3):
        pl.semaphore_signal(barrier, inc=1, device_id=(dev(x + d, y, c), z), device_id_type=MESH)
    for d in (1, 2, 3):
        pl.semaphore_signal(barrier, inc=1, device_id=(dev(x, y + d, c), z), device_id_type=MESH)
    for cp in loads:
        cp.wait()
    with jax.named_scope('bar'):
        pl.semaphore_wait(barrier, nm - 1 + 5)

    def rcopy(src, dst, ss, rs, to):
        return pltpu.make_async_remote_copy(
            src_ref=src, dst_ref=dst, send_sem=ss, recv_sem=rs,
            device_id=to, device_id_type=MESH)

    def s0_copy(r, w):
        cc, zz = member(r)
        g = pl.multiple_of((2 * zz + cc) * HEAD_SIZE, HEAD_SIZE)
        src = (k_ref, v_ref)[w].at[:, pl.ds(g, HEAD_SIZE)]
        off = pl.multiple_of(c * rows + z * piece, piece)
        return rcopy(src, kv.at[x, y, w, pl.ds(off, piece), :],
                     s0s.at[r, w], s0r.at[r, w], (dev(x, y, cc), zz))

    for r in range(1, nm):
        for w in range(2):
            s0_copy(r, w).start()

    other = pl.multiple_of((1 - c) * half, half)
    mine = pl.multiple_of(c * half, half)
    sib = (dev(x, y, 1 - c), z)
    sib_copies = [
        rcopy(lse_ref, slse, sbs.at[3], sbr.at[3], sib),
        rcopy(q_ref.at[:, pl.ds(other, half)], sq, sbs.at[0], sbr.at[0], sib),
        rcopy(do_ref.at[:, pl.ds(other, half)], sdo, sbs.at[1], sbr.at[1], sib),
        rcopy(o_ref.at[:, pl.ds(other, half)], so, sbs.at[2], sbr.at[2], sib),
    ]
    for cp in sib_copies:
        cp.start()

    own_off = pl.multiple_of(c * rows + z * piece, piece)
    own_g = pl.multiple_of((2 * z + c) * HEAD_SIZE, HEAD_SIZE)
    kv[x, y, 0, pl.ds(own_off, piece), :] = k_ref[:, pl.ds(own_g, HEAD_SIZE)]
    kv[x, y, 1, pl.ds(own_off, piece), :] = v_ref[:, pl.ds(own_g, HEAD_SIZE)]

    lane = lax.broadcasted_iota(jnp.int32, (blk, HEAD_SIZE), 1)
    slot = lane - (HEAD_SIZE - bo_ref.shape[0])

    def three(col, rest):
        hi = col.astype(BF).astype(F32)
        mid = (col - hi).astype(BF).astype(F32)
        lo = col - hi - mid
        return jnp.where(lane == 0, hi, jnp.where(lane == 1, mid, jnp.where(lane == 2, lo, rest))).astype(BF)

    chip_block = (x * 4 + y) * 4
    zero = jnp.zeros((blk, HEAD_SIZE), F32)
    lpad[...] = jnp.zeros_like(lpad)

    def prepare(qr, dor, orf, lr, col0, core):
        lpad[0:2 * RATIO, :] = lr[...]
        lt[...] = lpad[...].T
        for b in range(2):
            rs = pl.ds(b * blk, blk)
            dst = pl.ds(pl.multiple_of(core * rows + b * blk, blk), blk)
            therm = jnp.where(slot > bo_ref[chip_block + 2 * core + b], -BIG, zero)
            for h in range(RATIO):
                cols = pl.ds(pl.multiple_of(col0 + h * HEAD_SIZE, HEAD_SIZE), HEAD_SIZE)
                q = qr[rs, cols]
                do = dor[rs, cols]
                lse = jnp.where(c == 0, lt[rs, h:h + 1], lt[rs, RATIO + h:RATIO + h + 1])
                delta = jnp.sum(do.astype(F32) * orf[rs, cols].astype(F32), axis=1, keepdims=True)
                qa[h, dst, 0:HEAD_SIZE] = q
                qa[h, dst, HEAD_SIZE:] = three(lse * (-1.0 / SCALE), therm)
                doa[h, dst, 0:HEAD_SIZE] = do
                doa[h, dst, HEAD_SIZE:] = three(-delta, zero)
                tdst = pl.ds(pl.multiple_of(h * chip + core * rows + b * blk, blk), blk)
                qt[:, tdst] = q.astype(F32).T.astype(BF)
                dot_[:, tdst] = do.astype(F32).T.astype(BF)

    with jax.named_scope('prep0'):
        prepare(q_ref, do_ref, o_ref, lse_ref, mine, c)
    dqacc[...] = jnp.zeros_like(dqacc)
    lane_v = lax.broadcasted_iota(jnp.int32, (chip, HEAD_SIZE), 1)
    ones_tail = jnp.where(lane_v < 3, 1.0, 0.0).astype(BF)
    with jax.named_scope('sibwait'):
        for cp in sib_copies:
            cp.wait_recv()
    with jax.named_scope('prep1'):
        prepare(sq, sdo, so, slse, 0, 1 - c)

    with jax.named_scope('s0wait'):
        for r in range(1, nm):
            for w in range(2):
                s0_copy(r, w).wait_recv()

    def at(d, e):
        return kv.at[(x - d + 4) % 4, (y - e + 4) % 4]

    xp, xm = (dev(x + 1, y, c), z), (dev(x + 3, y, c), z)
    yp, ym = (dev(x, y + 1, c), z), (dev(x, y + 3, c), z)

    def ax(d, chunk):
        return rcopy(chunk, chunk, axs.at[d], axr.at[d], xp if d == 1 else xm)

    def fx(w, chunk):
        return rcopy(chunk.at[w], chunk.at[w], fxs.at[w], fxr.at[w], (xp, xm)[w])

    def ay(d, e, chunk):
        return rcopy(chunk, chunk, ays.at[d, e], ayr.at[d, e], yp if e == 1 else ym)

    def fy(d, w, chunk):
        return rcopy(chunk.at[w], chunk.at[w], fys.at[d, w], fyr.at[d, w], (yp, ym)[w])

    ax(1, at(0, 0)).start()
    ax(3, at(0, 0)).start()
    ay(0, 1, at(0, 0)).start()
    ay(0, 3, at(0, 0)).start()

    def compute(d, e, masked):
        xs, ys = (x - d + 4) % 4, (y - e + 4) % 4
        kb = (xs * 4 + ys) * 4
        for b in range(4):
            ktail[b * blk:(b + 1) * blk, :] = jnp.where(
                (lane < 3) | (slot == bo_ref[kb + b]), 1.0, zero).astype(BF)
        key = kv[xs, ys, 0]
        ka = jnp.concatenate([key, ktail[...]], axis=1)
        va = jnp.concatenate([kv[xs, ys, 1], ones_tail], axis=1)
        nt = (((1,), (1,)), ((), ()))
        for h in range(RATIO):
            sc = lax.dot_general(qa[h], ka, nt, preferred_element_type=F32)
            dp = lax.dot_general(doa[h], va, nt, preferred_element_type=F32)
            p = jnp.exp2(sc * (SCALE * LOG2E))
            if masked:
                row = lax.broadcasted_iota(jnp.int32, p.shape, 0)
                col = lax.broadcasted_iota(jnp.int32, p.shape, 1)
                p = jnp.where((col > row) & (col // blk == row // blk), 0.0, p)
            ds = (p * dp).astype(BF)
            pbig[h * chip:(h + 1) * chip, :] = p.astype(BF)
            dsbig[h * chip:(h + 1) * chip, :] = ds
            dqacc[h] += jnp.dot(ds, key, preferred_element_type=F32)
        pbuf[d, e, 0] = (jnp.dot(qt[...], dsbig[...], preferred_element_type=F32) * SCALE).astype(BF)
        pbuf[d, e, 1] = jnp.dot(dot_[...], pbig[...], preferred_element_type=F32).astype(BF)

    def relay(e, w):
        return rcopy(pbuf.at[2, e, w], ra.at[e, w], ras.at[e, w], rar.at[e, w], (xm, xp)[w])

    def near(d, e, w):
        i = (d - 1) // 2
        return rcopy(pbuf.at[d, e, w], r1.at[i, e, w], r1s.at[i, e, w], r1r.at[i, e, w], xm if d == 1 else xp)

    def r2_copy(e, w):
        return rcopy(s2.at[e, w], r2.at[e, w], r2s.at[e, w], r2r.at[e, w], (dev(x, y - e + 4, c), z))

    def relays(e):
        relay(e, 0).start()
        relay(e, 1).start()

    def plain(d, e):
        near(d, e, 1 if d == 1 else 0).start()

    def join(d, e):
        w = 0 if d == 1 else 1
        with jax.named_scope('ra'):
            relay(e, w).wait_recv()
        pbuf[d, e, w] = (pbuf[d, e, w].astype(F32) + ra[e, w].astype(F32)).astype(BF)
        near(d, e, w).start()

    def sum_x(e, w):
        with jax.named_scope('r1'):
            near(1, e, w).wait_recv()
            near(3, e, w).wait_recv()
        return pbuf[0, e, w].astype(F32) + r1[0, e, w].astype(F32) + r1[1, e, w].astype(F32)

    def combine(e):
        for w in range(2):
            s2[e, w] = sum_x(e, w).astype(BF)

    def got_x():
        ax(1, at(1, 0)).wait_recv()
        ay(1, 1, at(1, 0)).start()
        fx(0, at(1, 0)).start()
        ax(3, at(3, 0)).wait_recv()
        ay(3, 3, at(3, 0)).start()
        fx(1, at(3, 0)).start()
        ay(0, 1, at(0, 1)).wait_recv()

    def got_far_x():
        fx(0, at(2, 0)).wait_recv()
        fx(1, at(2, 0)).wait_recv()
        ay(2, 1, at(2, 0)).start()
        ay(2, 3, at(2, 0)).start()
        ay(3, 1, at(3, 0)).start()
        ay(1, 3, at(1, 0)).start()

    def got_y(d, e):
        ay(d, e, at(d, e)).wait_recv()

    def far_k(d):
        fy(d, 0, at(d, 1)).start()

    def far_v(d):
        fy(d, 1, at(d, 3)).start()

    def got_far_y(d):
        fy(d, 0, at(d, 2)).wait_recv()
        fy(d, 1, at(d, 2)).wait_recv()

    def r2_send(e):
        r2_copy(e, 0).start()
        r2_copy(e, 1).start()

    events = {
        1: lambda: got_x(),
        2: lambda: got_y(0, 3),
        3: lambda: got_far_x(),
        4: lambda: (got_y(1, 1), relays(0)),
        5: lambda: (got_y(3, 3), plain(1, 1)),
        6: lambda: (got_y(2, 1), far_k(2), plain(3, 3)),
        7: lambda: (got_y(2, 3), far_v(2), relays(1)),
        8: lambda: (got_y(3, 1), far_k(0), far_v(0), relays(3)),
        9: lambda: (got_y(1, 3), plain(3, 1), far_k(1), far_v(1), far_k(3), far_v(3)),
        10: lambda: (got_far_y(2), plain(1, 3), join(1, 1), join(3, 1)),
        11: lambda: (got_far_y(0), relays(2), join(3, 3), join(1, 3)),
        12: lambda: got_far_y(1),
        13: lambda: (got_far_y(3), combine(1)),
        14: lambda: (plain(3, 2), join(1, 2), plain(1, 2), join(3, 2), r2_send(1), combine(3)),
        15: lambda: (plain(1, 0), join(1, 0), r2_send(3)),
    }

    with jax.named_scope('comp0'):
        compute(0, 0, True)

    def step(t, carry):
        for g in range(4):
            @pl.when(t // 4 == g)
            def _():
                for k in range(max(1, 4 * g), 4 * g + 4):
                    @pl.when(t == k)
                    def _():
                        with jax.named_scope('ev%d' % k):
                            events[k]()
        with jax.named_scope('comp'):
            compute(pick(t, [o[0] for o in ORDER]), pick(t, [o[1] for o in ORDER]), False)
        return carry

    lax.fori_loop(1, 16, step, 0)
    plain(3, 0)
    join(3, 0)

    orow = pl.multiple_of((1 - c) * rows, rows)
    mrow = pl.multiple_of(c * rows, rows)
    with jax.named_scope('dq'):
        for h in range(RATIO):
            dqs[:, h * HEAD_SIZE:(h + 1) * HEAD_SIZE] = (dqacc[h, pl.ds(orow, rows), :] * SCALE).astype(BF)
        for h in range(RATIO):
            cols = pl.ds(pl.multiple_of(mine + h * HEAD_SIZE, HEAD_SIZE), HEAD_SIZE)
            dq_ref[:, cols] = (dqacc[h, pl.ds(mrow, rows), :] * SCALE).astype(BF)
    for w in range(2):
        s2[2, w] = sum_x(2, w).astype(BF)
        r2_copy(2, w).start()
    dq_copy = rcopy(dqs, dq_ref.at[:, pl.ds(mine, half)], dqss.at[0], dqsr.at[0], sib)
    dq_copy.start()

    def s4_copy(r, w):
        cc, zz = member(r)
        off = pl.multiple_of(cc * rows + zz * piece, piece)
        dst = (dk_ref, dv_ref)[w].at[:, pl.ds(own_g, HEAD_SIZE)]
        return rcopy(fin.at[w, pl.ds(off, piece), :], dst, s4s.at[r, w], s4r.at[r, w], (dev(x, y, cc), zz))

    for w in range(2):
        tot = sum_x(0, w)
        for e in (1, 3, 2):
            with jax.named_scope('r2w'):
                r2_copy(e, w).wait_recv()
            tot = tot + r2[e, w].astype(F32)
        fin[w] = tot.T.astype(BF)
        for r in range(1, nm):
            s4_copy(r, w).start()
    dk_ref[:, pl.ds(own_g, HEAD_SIZE)] = fin[0, pl.ds(own_off, piece), :]
    dv_ref[:, pl.ds(own_g, HEAD_SIZE)] = fin[1, pl.ds(own_off, piece), :]

    def s4_wait(r, w):
        m = (me - r + nm) % nm
        cc, zz = m // nz, m % nz
        g = pl.multiple_of((2 * zz + cc) * HEAD_SIZE, HEAD_SIZE)
        dst = (dk_ref, dv_ref)[w].at[:, pl.ds(g, HEAD_SIZE)]
        rcopy(fin.at[w, pl.ds(0, piece), :], dst, s4s.at[r, w], s4r.at[r, w], sib).wait_recv()

    with jax.named_scope('s4w'):
        for r in range(1, nm):
            for w in range(2):
                s4_wait(r, w)
    rcopy(dqs, dq_ref.at[:, pl.ds(other, half)], dqss.at[0], dqsr.at[0], sib).wait_recv()

    for r in range(1, nm):
        for w in range(2):
            s0_copy(r, w).wait_send()
            s4_copy(r, w).wait_send()
    for cp in sib_copies:
        cp.wait_send()
    dq_copy.wait_send()
    for d in (1, 3):
        ax(d, at(0, 0)).wait_send()
    for w in range(2):
        fx(w, at(0, 0)).wait_send()
        for e in (1, 2, 3):
            r2_copy(e, w).wait_send()
        for e in range(4):
            relay(e, w).wait_send()
            near(1, e, w).wait_send()
            near(3, e, w).wait_send()
        for d in range(4):
            fy(d, w, at(0, 0)).wait_send()
    for d in range(4):
        ay(d, 1, at(0, 0)).wait_send()
        ay(d, 3, at(0, 0)).wait_send()


def fused(nz, queries, keys, values, outputs, out_grad, log_norm, block_order):
    rows, piece = queries.shape[0], keys.shape[0]
    chip = 2 * rows
    half = RATIO * HEAD_SIZE
    nm = 2 * nz
    dma = pltpu.SemaphoreType.DMA
    vm = pl.BlockSpec(memory_space=pltpu.VMEM)
    hbm = pl.BlockSpec(memory_space=pltpu.HBM)
    return pl.pallas_call(
        functools.partial(kernel, nz),
        out_shape=(
            jax.ShapeDtypeStruct(queries.shape, BF),
            jax.ShapeDtypeStruct(keys.shape, BF),
            jax.ShapeDtypeStruct(values.shape, BF),
        ),
        in_specs=[hbm] * 7,
        out_specs=(vm, vm, vm),
        scratch_shapes=[
            pltpu.VMEM(queries.shape, BF),
            pltpu.VMEM(keys.shape, BF),
            pltpu.VMEM(values.shape, BF),
            pltpu.VMEM(outputs.shape, BF),
            pltpu.VMEM(out_grad.shape, BF),
            pltpu.VMEM(log_norm.shape, F32),
            pltpu.SMEM(block_order.shape, jnp.int32),
            pltpu.VMEM((4, 4, 2, chip, HEAD_SIZE), BF),
            pltpu.VMEM((rows, half), BF),
            pltpu.VMEM((rows, half), BF),
            pltpu.VMEM((rows, half), BF),
            pltpu.VMEM(log_norm.shape, F32),
            pltpu.VMEM((HEAD_SIZE, rows), F32),
            pltpu.VMEM((rows, HEAD_SIZE), F32),
            pltpu.VMEM((RATIO, chip, 2 * HEAD_SIZE), BF),
            pltpu.VMEM((RATIO, chip, 2 * HEAD_SIZE), BF),
            pltpu.VMEM((HEAD_SIZE, RATIO * chip), BF),
            pltpu.VMEM((HEAD_SIZE, RATIO * chip), BF),
            pltpu.VMEM((chip, HEAD_SIZE), BF),
            pltpu.VMEM((RATIO * chip, chip), BF),
            pltpu.VMEM((RATIO * chip, chip), BF),
            pltpu.VMEM((RATIO, chip, HEAD_SIZE), F32),
            pltpu.VMEM((4, 4, 2, HEAD_SIZE, chip), BF),
            pltpu.VMEM((2, 4, 2, HEAD_SIZE, chip), BF),
            pltpu.VMEM((4, 2, HEAD_SIZE, chip), BF),
            pltpu.VMEM((4, 2, HEAD_SIZE, chip), BF),
            pltpu.VMEM((4, 2, HEAD_SIZE, chip), BF),
            pltpu.VMEM((2, chip, HEAD_SIZE), BF),
            pltpu.VMEM((rows, half), BF),
            dma((7,)),
            dma((nm, 2)), dma((nm, 2)), dma((4,)), dma((4,)),
            dma((4,)), dma((4,)), dma((4, 4)), dma((4, 4)),
            dma((2,)), dma((2,)), dma((4, 2)), dma((4, 2)),
            dma((2, 4, 2)), dma((2, 4, 2)), dma((4, 2)), dma((4, 2)),
            dma((4, 2)), dma((4, 2)), dma((nm, 2)), dma((nm, 2)), dma((1,)), dma((1,)),
        ],
        compiler_params=pltpu.CompilerParams(
            collective_id=0, has_side_effects=True, vmem_limit_bytes=40 * 1024 * 1024),
    )(*(pltpu.with_memory_space_constraint(a, pltpu.HBM) for a in (
        queries, keys, values, outputs, out_grad, log_norm, block_order)))


def solution(mesh):
    in_specs = (
        P("seq", "head"),
        P(("seq", "head"), None),
        P(("seq", "head"), None),
        P("seq", "head"),
        P("seq", "head"),
        P("head", "seq"),
        P(),
    )
    out_specs = (P("seq", "head"), P(("seq", "head"), None), P(("seq", "head"), None))
    return jax.shard_map(
        functools.partial(fused, mesh.shape["head"]), mesh=mesh,
        in_specs=in_specs, out_specs=out_specs, check_vma=False)
```

```python
import functools

import jax
import jax.numpy as jnp
from jax import lax
from jax.experimental import pallas as pl
from jax.experimental.pallas import tpu as pltpu
from jax.sharding import PartitionSpec as P

HEAD_SIZE = 128
RATIO = 4
SCALE = HEAD_SIZE ** (-0.5)
LOG2E = 1.4426950408889634
BIG = 131072.0
MESH = pl.DeviceIdType.MESH
BF = jnp.bfloat16
F32 = jnp.float32


ORDER = (
    (0, 0), (0, 1), (0, 3), (2, 0), (1, 1), (3, 3), (2, 1), (2, 3),
    (3, 1), (1, 3), (2, 2), (0, 2), (1, 2), (3, 2), (1, 0), (3, 0),
)


def pick(t, values):
    out = values[0]
    for i, v in enumerate(values):
        out = jnp.where(t == i, v, out)
    return out


def kernel(
    nz,
    qh, kh, vh, oh, doh, lseh, boh,
    dq_ref, dk_ref, dv_ref,
    q_ref, k_ref, v_ref, o_ref, do_ref, lse_ref, bo_ref,
    kv, sq, sdo, so, slse, lpad, lt, qa, doa, qt, dot_, ktail, pbig, dsbig, dqacc,
    pbuf, r1, ra, s2, r2, fin, dqs,
    ins, s0s, s0r, sbs, sbr, axs, axr, ays, ayr, fxs, fxr, fys, fyr,
    r1s, r1r, ras, rar, r2s, r2r, s4s, s4r, dqss, dqsr,
):
    s = lax.axis_index("seq")
    z = lax.axis_index("head")
    x, y, c = s // 8, (s // 2) % 4, s % 2
    rows = q_ref.shape[0]
    piece = k_ref.shape[0]
    chip = 2 * rows
    blk = rows // 2
    half = RATIO * HEAD_SIZE
    nm = 2 * nz

    def dev(xx, yy, cc):
        return ((xx % 4) * 4 + (yy % 4)) * 2 + cc

    way = 1 - 2 * c

    def up(p, n):
        return (p + way * n + 4) % 4

    me = c * nz + z

    def member(r):
        m = (me + r) % nm
        return m // nz, m % nz

    loads = [
        pltpu.make_async_copy(src, dst, ins.at[i])
        for i, (src, dst) in enumerate((
            (kh, k_ref), (vh, v_ref), (qh, q_ref), (doh, do_ref), (oh, o_ref), (lseh, lse_ref), (boh, bo_ref)))
    ]
    barrier = pltpu.get_barrier_semaphore()
    for r in range(1, nm):
        cc, zz = member(r)
        pl.semaphore_signal(barrier, inc=1, device_id=(dev(x, y, cc), zz), device_id_type=MESH)
    for d in (1, 3):
        pl.semaphore_signal(barrier, inc=1, device_id=(dev(up(x, d), y, c), z), device_id_type=MESH)
    for d in (1, 2, 3):
        pl.semaphore_signal(barrier, inc=1, device_id=(dev(x, up(y, d), c), z), device_id_type=MESH)
    for cp in loads:
        cp.start()
    for cp in loads:
        cp.wait()
    with jax.named_scope('bar'):
        pl.semaphore_wait(barrier, nm - 1 + 5)

    def rcopy(src, dst, ss, rs, to):
        return pltpu.make_async_remote_copy(
            src_ref=src, dst_ref=dst, send_sem=ss, recv_sem=rs,
            device_id=to, device_id_type=MESH)

    def s0_copy(r, w):
        cc, zz = member(r)
        g = pl.multiple_of((2 * zz + cc) * HEAD_SIZE, HEAD_SIZE)
        src = (k_ref, v_ref)[w].at[:, pl.ds(g, HEAD_SIZE)]
        off = pl.multiple_of(c * rows + z * piece, piece)
        return rcopy(src, kv.at[x, y, w, pl.ds(off, piece), :],
                     s0s.at[r, w], s0r.at[r, w], (dev(x, y, cc), zz))

    for r in range(1, nm):
        for w in range(2):
            s0_copy(r, w).start()

    other = pl.multiple_of((1 - c) * half, half)
    mine = pl.multiple_of(c * half, half)
    sib = (dev(x, y, 1 - c), z)
    sib_copies = [
        rcopy(lse_ref, slse, sbs.at[3], sbr.at[3], sib),
        rcopy(q_ref.at[:, pl.ds(other, half)], sq, sbs.at[0], sbr.at[0], sib),
        rcopy(do_ref.at[:, pl.ds(other, half)], sdo, sbs.at[1], sbr.at[1], sib),
        rcopy(o_ref.at[:, pl.ds(other, half)], so, sbs.at[2], sbr.at[2], sib),
    ]
    for cp in sib_copies:
        cp.start()

    own_off = pl.multiple_of(c * rows + z * piece, piece)
    own_g = pl.multiple_of((2 * z + c) * HEAD_SIZE, HEAD_SIZE)
    kv[x, y, 0, pl.ds(own_off, piece), :] = k_ref[:, pl.ds(own_g, HEAD_SIZE)]
    kv[x, y, 1, pl.ds(own_off, piece), :] = v_ref[:, pl.ds(own_g, HEAD_SIZE)]

    lane = lax.broadcasted_iota(jnp.int32, (blk, HEAD_SIZE), 1)
    slot = lane - (HEAD_SIZE - bo_ref.shape[0])

    def three(col, rest):
        hi = col.astype(BF).astype(F32)
        mid = (col - hi).astype(BF).astype(F32)
        lo = col - hi - mid
        return jnp.where(lane == 0, hi, jnp.where(lane == 1, mid, jnp.where(lane == 2, lo, rest))).astype(BF)

    chip_block = (x * 4 + y) * 4
    zero = jnp.zeros((blk, HEAD_SIZE), F32)
    lpad[...] = jnp.zeros_like(lpad)

    def prepare(qr, dor, orf, lr, col0, core):
        lpad[0:2 * RATIO, :] = lr[...]
        lt[...] = lpad[...].T
        for b in range(2):
            rs = pl.ds(b * blk, blk)
            dst = pl.ds(pl.multiple_of(core * rows + b * blk, blk), blk)
            therm = jnp.where(slot > bo_ref[chip_block + 2 * core + b], -BIG, zero)
            for h in range(RATIO):
                cols = pl.ds(pl.multiple_of(col0 + h * HEAD_SIZE, HEAD_SIZE), HEAD_SIZE)
                q = qr[rs, cols]
                do = dor[rs, cols]
                lse = jnp.where(c == 0, lt[rs, h:h + 1], lt[rs, RATIO + h:RATIO + h + 1])
                delta = jnp.sum(do.astype(F32) * orf[rs, cols].astype(F32), axis=1, keepdims=True)
                qa[h, dst, 0:HEAD_SIZE] = q
                qa[h, dst, HEAD_SIZE:] = three(lse * (-1.0 / SCALE), therm)
                doa[h, dst, 0:HEAD_SIZE] = do
                doa[h, dst, HEAD_SIZE:] = three(-delta, zero)
                tdst = pl.ds(pl.multiple_of(h * chip + core * rows + b * blk, blk), blk)
                qt[:, tdst] = q.astype(F32).T.astype(BF)
                dot_[:, tdst] = do.astype(F32).T.astype(BF)

    with jax.named_scope('prep0'):
        prepare(q_ref, do_ref, o_ref, lse_ref, mine, c)
    dqacc[...] = jnp.zeros_like(dqacc)
    lane_v = lax.broadcasted_iota(jnp.int32, (chip, HEAD_SIZE), 1)
    ones_tail = jnp.where(lane_v < 3, 1.0, 0.0).astype(BF)
    with jax.named_scope('s0wait'):
        for r in range(1, nm):
            for w in range(2):
                s0_copy(r, w).wait_recv()

    def at(d, e):
        return kv.at[up(x, -d), up(y, -e)]

    xp, xm = (dev(up(x, 1), y, c), z), (dev(up(x, -1), y, c), z)
    yp, ym = (dev(x, up(y, 1), c), z), (dev(x, up(y, -1), c), z)

    def ax(d, chunk):
        return rcopy(chunk, chunk, axs.at[d], axr.at[d], xp if d == 1 else xm)

    def fx(w, chunk):
        return rcopy(chunk.at[w], chunk.at[w], fxs.at[w], fxr.at[w], (xp, xm)[w])

    def ay(d, e, chunk):
        return rcopy(chunk, chunk, ays.at[d, e], ayr.at[d, e], yp if e == 1 else ym)

    def fy(d, w, chunk):
        return rcopy(chunk.at[w], chunk.at[w], fys.at[d, w], fyr.at[d, w], (yp, ym)[w])

    ax(1, at(0, 0)).start()
    ax(3, at(0, 0)).start()
    ay(0, 1, at(0, 0)).start()
    ay(0, 3, at(0, 0)).start()

    with jax.named_scope('sibwait'):
        for cp in sib_copies:
            cp.wait_recv()
    with jax.named_scope('prep1'):
        prepare(sq, sdo, so, slse, 0, 1 - c)

    def compute(d, e, masked):
        xs, ys = up(x, -d), up(y, -e)
        kb = (xs * 4 + ys) * 4
        for b in range(4):
            ktail[b * blk:(b + 1) * blk, :] = jnp.where(
                (lane < 3) | (slot == bo_ref[kb + b]), 1.0, zero).astype(BF)
        key = kv[xs, ys, 0]
        ka = jnp.concatenate([key, ktail[...]], axis=1)
        va = jnp.concatenate([kv[xs, ys, 1], ones_tail], axis=1)
        nt = (((1,), (1,)), ((), ()))
        for h in range(RATIO):
            sc = lax.dot_general(qa[h], ka, nt, preferred_element_type=F32)
            dp = lax.dot_general(doa[h], va, nt, preferred_element_type=F32)
            p = jnp.exp2(sc * (SCALE * LOG2E))
            if masked:
                row = lax.broadcasted_iota(jnp.int32, p.shape, 0)
                col = lax.broadcasted_iota(jnp.int32, p.shape, 1)
                p = jnp.where((col > row) & (col // blk == row // blk), 0.0, p)
            ds = (p * dp).astype(BF)
            pbig[h * chip:(h + 1) * chip, :] = p.astype(BF)
            dsbig[h * chip:(h + 1) * chip, :] = ds
            dqacc[h] += jnp.dot(ds, key, preferred_element_type=F32)
        pbuf[d, e, 0] = (jnp.dot(qt[...], dsbig[...], preferred_element_type=F32) * SCALE).astype(BF)
        pbuf[d, e, 1] = jnp.dot(dot_[...], pbig[...], preferred_element_type=F32).astype(BF)

    def relay(e, w):
        return rcopy(pbuf.at[2, e, w], ra.at[e, w], ras.at[e, w], rar.at[e, w], (xm, xp)[w])

    def near(d, e, w):
        i = (d - 1) // 2
        return rcopy(pbuf.at[d, e, w], r1.at[i, e, w], r1s.at[i, e, w], r1r.at[i, e, w], xm if d == 1 else xp)

    def r2_copy(e, w):
        return rcopy(s2.at[e, w], r2.at[e, w], r2s.at[e, w], r2r.at[e, w], (dev(x, up(y, -e), c), z))

    def relays(e):
        relay(e, 0).start()
        relay(e, 1).start()

    def plain(d, e):
        near(d, e, 1 if d == 1 else 0).start()

    def join(d, e):
        w = 0 if d == 1 else 1
        with jax.named_scope('ra'):
            relay(e, w).wait_recv()
        pbuf[d, e, w] = (pbuf[d, e, w].astype(F32) + ra[e, w].astype(F32)).astype(BF)
        near(d, e, w).start()

    def sum_x(e, w):
        with jax.named_scope('r1'):
            near(1, e, w).wait_recv()
            near(3, e, w).wait_recv()
        return pbuf[0, e, w].astype(F32) + r1[0, e, w].astype(F32) + r1[1, e, w].astype(F32)

    def combine(e):
        for w in range(2):
            s2[e, w] = sum_x(e, w).astype(BF)

    def got_x():
        ax(1, at(1, 0)).wait_recv()
        ay(1, 1, at(1, 0)).start()
        fx(0, at(1, 0)).start()
        ax(3, at(3, 0)).wait_recv()
        ay(3, 3, at(3, 0)).start()
        fx(1, at(3, 0)).start()
        ay(0, 1, at(0, 1)).wait_recv()

    def got_far_x():
        fx(0, at(2, 0)).wait_recv()
        fx(1, at(2, 0)).wait_recv()
        ay(2, 1, at(2, 0)).start()
        ay(2, 3, at(2, 0)).start()
        ay(3, 1, at(3, 0)).start()
        ay(1, 3, at(1, 0)).start()

    def got_y(d, e):
        ay(d, e, at(d, e)).wait_recv()

    def far_k(d):
        fy(d, 0, at(d, 1)).start()

    def far_v(d):
        fy(d, 1, at(d, 3)).start()

    def got_far_y(d):
        fy(d, 0, at(d, 2)).wait_recv()
        fy(d, 1, at(d, 2)).wait_recv()

    def r2_send(e):
        r2_copy(e, 0).start()
        r2_copy(e, 1).start()

    events = {
        1: lambda: got_x(),
        2: lambda: got_y(0, 3),
        3: lambda: got_far_x(),
        4: lambda: (got_y(1, 1), relays(0)),
        5: lambda: (got_y(3, 3), plain(1, 1)),
        6: lambda: (got_y(2, 1), far_k(2), plain(3, 3)),
        7: lambda: (got_y(2, 3), far_v(2), relays(1)),
        8: lambda: (got_y(3, 1), far_k(0), far_v(0), relays(3)),
        9: lambda: (got_y(1, 3), plain(3, 1), far_k(1), far_v(1), far_k(3), far_v(3)),
        10: lambda: (got_far_y(2), plain(1, 3), join(1, 1), join(3, 1)),
        11: lambda: (got_far_y(0), relays(2), join(3, 3), join(1, 3)),
        12: lambda: got_far_y(1),
        13: lambda: (got_far_y(3), combine(1)),
        14: lambda: (plain(3, 2), join(1, 2), plain(1, 2), join(3, 2), r2_send(1), combine(3)),
        15: lambda: (plain(1, 0), join(1, 0), r2_send(3)),
    }

    with jax.named_scope('comp0'):
        compute(0, 0, True)

    def step(t, carry):
        for g in range(4):
            @pl.when(t // 4 == g)
            def _():
                for k in range(max(1, 4 * g), 4 * g + 4):
                    @pl.when(t == k)
                    def _():
                        with jax.named_scope('ev%d' % k):
                            events[k]()
        with jax.named_scope('comp'):
            compute(pick(t, [o[0] for o in ORDER]), pick(t, [o[1] for o in ORDER]), False)
        return carry

    lax.fori_loop(1, 16, step, 0)
    plain(3, 0)
    join(3, 0)

    orow = pl.multiple_of((1 - c) * rows, rows)
    mrow = pl.multiple_of(c * rows, rows)
    with jax.named_scope('dq'):
        for h in range(RATIO):
            dqs[:, h * HEAD_SIZE:(h + 1) * HEAD_SIZE] = (dqacc[h, pl.ds(orow, rows), :] * SCALE).astype(BF)
        for h in range(RATIO):
            cols = pl.ds(pl.multiple_of(mine + h * HEAD_SIZE, HEAD_SIZE), HEAD_SIZE)
            dq_ref[:, cols] = (dqacc[h, pl.ds(mrow, rows), :] * SCALE).astype(BF)
    for w in range(2):
        s2[2, w] = sum_x(2, w).astype(BF)
        r2_copy(2, w).start()
    dq_copy = rcopy(dqs, dq_ref.at[:, pl.ds(mine, half)], dqss.at[0], dqsr.at[0], sib)
    dq_copy.start()

    def s4_copy(r, w):
        cc, zz = member(r)
        off = pl.multiple_of(cc * rows + zz * piece, piece)
        dst = (dk_ref, dv_ref)[w].at[:, pl.ds(own_g, HEAD_SIZE)]
        return rcopy(fin.at[w, pl.ds(off, piece), :], dst, s4s.at[r, w], s4r.at[r, w], (dev(x, y, cc), zz))

    for w in range(2):
        tot = sum_x(0, w)
        for e in (1, 3, 2):
            with jax.named_scope('r2w'):
                r2_copy(e, w).wait_recv()
            tot = tot + r2[e, w].astype(F32)
        fin[w] = tot.T.astype(BF)
        for r in range(1, nm):
            s4_copy(r, w).start()
    dk_ref[:, pl.ds(own_g, HEAD_SIZE)] = fin[0, pl.ds(own_off, piece), :]
    dv_ref[:, pl.ds(own_g, HEAD_SIZE)] = fin[1, pl.ds(own_off, piece), :]

    def s4_wait(r, w):
        m = (me - r + nm) % nm
        cc, zz = m // nz, m % nz
        g = pl.multiple_of((2 * zz + cc) * HEAD_SIZE, HEAD_SIZE)
        dst = (dk_ref, dv_ref)[w].at[:, pl.ds(g, HEAD_SIZE)]
        rcopy(fin.at[w, pl.ds(0, piece), :], dst, s4s.at[r, w], s4r.at[r, w], sib).wait_recv()

    with jax.named_scope('s4w'):
        for r in range(1, nm):
            for w in range(2):
                s4_wait(r, w)
    rcopy(dqs, dq_ref.at[:, pl.ds(other, half)], dqss.at[0], dqsr.at[0], sib).wait_recv()

    for r in range(1, nm):
        for w in range(2):
            s0_copy(r, w).wait_send()
            s4_copy(r, w).wait_send()
    for cp in sib_copies:
        cp.wait_send()
    dq_copy.wait_send()
    for d in (1, 3):
        ax(d, at(0, 0)).wait_send()
    for w in range(2):
        fx(w, at(0, 0)).wait_send()
        for e in (1, 2, 3):
            r2_copy(e, w).wait_send()
        for e in range(4):
            relay(e, w).wait_send()
            near(1, e, w).wait_send()
            near(3, e, w).wait_send()
        for d in range(4):
            fy(d, w, at(0, 0)).wait_send()
    for d in range(4):
        ay(d, 1, at(0, 0)).wait_send()
        ay(d, 3, at(0, 0)).wait_send()


def fused(nz, queries, keys, values, outputs, out_grad, log_norm, block_order):
    rows, piece = queries.shape[0], keys.shape[0]
    chip = 2 * rows
    half = RATIO * HEAD_SIZE
    nm = 2 * nz
    dma = pltpu.SemaphoreType.DMA
    vm = pl.BlockSpec(memory_space=pltpu.VMEM)
    hbm = pl.BlockSpec(memory_space=pltpu.HBM)
    return pl.pallas_call(
        functools.partial(kernel, nz),
        out_shape=(
            jax.ShapeDtypeStruct(queries.shape, BF),
            jax.ShapeDtypeStruct(keys.shape, BF),
            jax.ShapeDtypeStruct(values.shape, BF),
        ),
        in_specs=[hbm] * 7,
        out_specs=(vm, vm, vm),
        scratch_shapes=[
            pltpu.VMEM(queries.shape, BF),
            pltpu.VMEM(keys.shape, BF),
            pltpu.VMEM(values.shape, BF),
            pltpu.VMEM(outputs.shape, BF),
            pltpu.VMEM(out_grad.shape, BF),
            pltpu.VMEM(log_norm.shape, F32),
            pltpu.SMEM(block_order.shape, jnp.int32),
            pltpu.VMEM((4, 4, 2, chip, HEAD_SIZE), BF),
            pltpu.VMEM((rows, half), BF),
            pltpu.VMEM((rows, half), BF),
            pltpu.VMEM((rows, half), BF),
            pltpu.VMEM(log_norm.shape, F32),
            pltpu.VMEM((HEAD_SIZE, rows), F32),
            pltpu.VMEM((rows, HEAD_SIZE), F32),
            pltpu.VMEM((RATIO, chip, 2 * HEAD_SIZE), BF),
            pltpu.VMEM((RATIO, chip, 2 * HEAD_SIZE), BF),
            pltpu.VMEM((HEAD_SIZE, RATIO * chip), BF),
            pltpu.VMEM((HEAD_SIZE, RATIO * chip), BF),
            pltpu.VMEM((chip, HEAD_SIZE), BF),
            pltpu.VMEM((RATIO * chip, chip), BF),
            pltpu.VMEM((RATIO * chip, chip), BF),
            pltpu.VMEM((RATIO, chip, HEAD_SIZE), F32),
            pltpu.VMEM((4, 4, 2, HEAD_SIZE, chip), BF),
            pltpu.VMEM((2, 4, 2, HEAD_SIZE, chip), BF),
            pltpu.VMEM((4, 2, HEAD_SIZE, chip), BF),
            pltpu.VMEM((4, 2, HEAD_SIZE, chip), BF),
            pltpu.VMEM((4, 2, HEAD_SIZE, chip), BF),
            pltpu.VMEM((2, chip, HEAD_SIZE), BF),
            pltpu.VMEM((rows, half), BF),
            dma((7,)),
            dma((nm, 2)), dma((nm, 2)), dma((4,)), dma((4,)),
            dma((4,)), dma((4,)), dma((4, 4)), dma((4, 4)),
            dma((2,)), dma((2,)), dma((4, 2)), dma((4, 2)),
            dma((2, 4, 2)), dma((2, 4, 2)), dma((4, 2)), dma((4, 2)),
            dma((4, 2)), dma((4, 2)), dma((nm, 2)), dma((nm, 2)), dma((1,)), dma((1,)),
        ],
        compiler_params=pltpu.CompilerParams(
            collective_id=0, has_side_effects=True, vmem_limit_bytes=40 * 1024 * 1024),
    )(*(pltpu.with_memory_space_constraint(a, pltpu.HBM) for a in (
        queries, keys, values, outputs, out_grad, log_norm, block_order)))


def solution(mesh):
    in_specs = (
        P("seq", "head"),
        P(("seq", "head"), None),
        P(("seq", "head"), None),
        P("seq", "head"),
        P("seq", "head"),
        P("head", "seq"),
        P(),
    )
    out_specs = (P("seq", "head"), P(("seq", "head"), None), P(("seq", "head"), None))
    return jax.shard_map(
        functools.partial(fused, mesh.shape["head"]), mesh=mesh,
        in_specs=in_specs, out_specs=out_specs, check_vma=False)
```

```python
import functools

import jax
import jax.numpy as jnp
from jax import lax
from jax.experimental import pallas as pl
from jax.experimental.pallas import tpu as pltpu
from jax.sharding import PartitionSpec as P

HEAD_SIZE = 128
RATIO = 4
SCALE = HEAD_SIZE ** (-0.5)
LOG2E = 1.4426950408889634
BIG = 131072.0
MESH = pl.DeviceIdType.MESH
BF = jnp.bfloat16
F32 = jnp.float32


ORDER = (
    (0, 0), (0, 1), (0, 3), (2, 0), (1, 1), (3, 3), (2, 1), (2, 3),
    (3, 1), (1, 3), (2, 2), (0, 2), (1, 2), (3, 2), (1, 0), (3, 0),
)


def pick(t, values):
    out = values[0]
    for i, v in enumerate(values):
        out = jnp.where(t == i, v, out)
    return out


def kernel(
    nz,
    qh, kh, vh, oh, doh, lseh, boh,
    dq_ref, dk_ref, dv_ref,
    q_ref, k_ref, v_ref, o_ref, do_ref, lse_ref, bo_ref,
    kv, sq, sdo, so, slse, lpad, lt, qa, doa, qt, dot_, ktail, pbig, dsbig, dqacc,
    pbuf, r1, ra, s2, r2, fin, dqs,
    ins, s0s, s0r, sbs, sbr, axs, axr, ays, ayr, fxs, fxr, fys, fyr,
    r1s, r1r, ras, rar, r2s, r2r, s4s, s4r, dqss, dqsr,
):
    s = lax.axis_index("seq")
    z = lax.axis_index("head")
    x, y, c = s // 8, (s // 2) % 4, s % 2
    rows = q_ref.shape[0]
    piece = k_ref.shape[0]
    chip = 2 * rows
    blk = rows // 2
    half = RATIO * HEAD_SIZE
    nm = 2 * nz

    def dev(xx, yy, cc):
        return ((xx % 4) * 4 + (yy % 4)) * 2 + cc

    way = 1 - 2 * c

    def up(p, n):
        return (p + way * n + 4) % 4

    me = c * nz + z

    def member(r):
        m = (me + r) % nm
        return m // nz, m % nz

    loads = [
        pltpu.make_async_copy(src, dst, ins.at[i])
        for i, (src, dst) in enumerate((
            (kh, k_ref), (vh, v_ref), (qh, q_ref), (doh, do_ref), (oh, o_ref), (lseh, lse_ref), (boh, bo_ref)))
    ]
    barrier = pltpu.get_barrier_semaphore()
    for r in range(1, nm):
        cc, zz = member(r)
        pl.semaphore_signal(barrier, inc=1, device_id=(dev(x, y, cc), zz), device_id_type=MESH)
    for d in (1, 3):
        pl.semaphore_signal(barrier, inc=1, device_id=(dev(up(x, d), y, c), z), device_id_type=MESH)
    for d in (1, 2, 3):
        pl.semaphore_signal(barrier, inc=1, device_id=(dev(x, up(y, d), c), z), device_id_type=MESH)
    for cp in loads:
        cp.start()
    for cp in loads:
        cp.wait()
    with jax.named_scope('bar'):
        pl.semaphore_wait(barrier, nm - 1 + 5)

    def rcopy(src, dst, ss, rs, to):
        return pltpu.make_async_remote_copy(
            src_ref=src, dst_ref=dst, send_sem=ss, recv_sem=rs,
            device_id=to, device_id_type=MESH)

    def s0_copy(r, w):
        cc, zz = member(r)
        g = pl.multiple_of((2 * zz + cc) * HEAD_SIZE, HEAD_SIZE)
        src = (k_ref, v_ref)[w].at[:, pl.ds(g, HEAD_SIZE)]
        off = pl.multiple_of(c * rows + z * piece, piece)
        return rcopy(src, kv.at[x, y, w, pl.ds(off, piece), :],
                     s0s.at[r, w], s0r.at[r, w], (dev(x, y, cc), zz))

    for r in range(1, nm):
        for w in range(2):
            s0_copy(r, w).start()

    other = pl.multiple_of((1 - c) * half, half)
    mine = pl.multiple_of(c * half, half)
    sib = (dev(x, y, 1 - c), z)
    sib_copies = [
        rcopy(lse_ref, slse, sbs.at[3], sbr.at[3], sib),
        rcopy(q_ref.at[:, pl.ds(other, half)], sq, sbs.at[0], sbr.at[0], sib),
        rcopy(do_ref.at[:, pl.ds(other, half)], sdo, sbs.at[1], sbr.at[1], sib),
        rcopy(o_ref.at[:, pl.ds(other, half)], so, sbs.at[2], sbr.at[2], sib),
    ]
    for cp in sib_copies:
        cp.start()

    own_off = pl.multiple_of(c * rows + z * piece, piece)
    own_g = pl.multiple_of((2 * z + c) * HEAD_SIZE, HEAD_SIZE)
    kv[x, y, 0, pl.ds(own_off, piece), :] = k_ref[:, pl.ds(own_g, HEAD_SIZE)]
    kv[x, y, 1, pl.ds(own_off, piece), :] = v_ref[:, pl.ds(own_g, HEAD_SIZE)]

    lane = lax.broadcasted_iota(jnp.int32, (blk, HEAD_SIZE), 1)
    slot = lane - (HEAD_SIZE - bo_ref.shape[0])

    def three(col, rest):
        hi = col.astype(BF).astype(F32)
        mid = (col - hi).astype(BF).astype(F32)
        lo = col - hi - mid
        return jnp.where(lane == 0, hi, jnp.where(lane == 1, mid, jnp.where(lane == 2, lo, rest))).astype(BF)

    chip_block = (x * 4 + y) * 4
    zero = jnp.zeros((blk, HEAD_SIZE), F32)
    lpad[...] = jnp.zeros_like(lpad)

    def prepare(qr, dor, orf, lr, col0, core):
        lpad[0:2 * RATIO, :] = lr[...]
        lt[...] = lpad[...].T
        for b in range(2):
            rs = pl.ds(b * blk, blk)
            dst = pl.ds(pl.multiple_of(core * rows + b * blk, blk), blk)
            therm = jnp.where(slot > bo_ref[chip_block + 2 * core + b], -BIG, zero)
            for h in range(RATIO):
                cols = pl.ds(pl.multiple_of(col0 + h * HEAD_SIZE, HEAD_SIZE), HEAD_SIZE)
                q = qr[rs, cols]
                do = dor[rs, cols]
                lse = jnp.where(c == 0, lt[rs, h:h + 1], lt[rs, RATIO + h:RATIO + h + 1])
                delta = jnp.sum(do.astype(F32) * orf[rs, cols].astype(F32), axis=1, keepdims=True)
                qa[h, dst, 0:HEAD_SIZE] = q
                qa[h, dst, HEAD_SIZE:] = three(lse * (-1.0 / SCALE), therm)
                doa[h, dst, 0:HEAD_SIZE] = do
                doa[h, dst, HEAD_SIZE:] = three(-delta, zero)
                tdst = pl.ds(pl.multiple_of(h * chip + core * rows + b * blk, blk), blk)
                qt[:, tdst] = q.astype(F32).T.astype(BF)
                dot_[:, tdst] = do.astype(F32).T.astype(BF)

    with jax.named_scope('prep0'):
        prepare(q_ref, do_ref, o_ref, lse_ref, mine, c)
    dqacc[...] = jnp.zeros_like(dqacc)
    lane_v = lax.broadcasted_iota(jnp.int32, (chip, HEAD_SIZE), 1)
    ones_tail = jnp.where(lane_v < 3, 1.0, 0.0).astype(BF)
    with jax.named_scope('s0wait'):
        for r in range(1, nm):
            for w in range(2):
                s0_copy(r, w).wait_recv()

    def at(d, e):
        return kv.at[up(x, -d), up(y, -e)]

    xp, xm = (dev(up(x, 1), y, c), z), (dev(up(x, -1), y, c), z)
    yp, ym = (dev(x, up(y, 1), c), z), (dev(x, up(y, -1), c), z)

    def ax(d, chunk):
        return rcopy(chunk, chunk, axs.at[d], axr.at[d], xp if d == 1 else xm)

    def fx(w, chunk):
        return rcopy(chunk.at[w], chunk.at[w], fxs.at[w], fxr.at[w], (xp, xm)[w])

    def ay(d, e, chunk):
        return rcopy(chunk, chunk, ays.at[d, e], ayr.at[d, e], yp if e == 1 else ym)

    def fy(d, w, chunk):
        return rcopy(chunk.at[w], chunk.at[w], fys.at[d, w], fyr.at[d, w], (yp, ym)[w])

    ax(1, at(0, 0)).start()
    ax(3, at(0, 0)).start()
    ay(0, 1, at(0, 0)).start()
    ay(0, 3, at(0, 0)).start()

    with jax.named_scope('sibwait'):
        for cp in sib_copies:
            cp.wait_recv()
    with jax.named_scope('prep1'):
        prepare(sq, sdo, so, slse, 0, 1 - c)

    def compute(d, e, masked):
        xs, ys = up(x, -d), up(y, -e)
        kb = (xs * 4 + ys) * 4
        for b in range(4):
            ktail[b * blk:(b + 1) * blk, :] = jnp.where(
                (lane < 3) | (slot == bo_ref[kb + b]), 1.0, zero).astype(BF)
        key = kv[xs, ys, 0]
        ka = jnp.concatenate([key, ktail[...]], axis=1)
        va = jnp.concatenate([kv[xs, ys, 1], ones_tail], axis=1)
        nt = (((1,), (1,)), ((), ()))
        for h in range(RATIO):
            sc = lax.dot_general(qa[h], ka, nt, preferred_element_type=F32)
            dp = lax.dot_general(doa[h], va, nt, preferred_element_type=F32)
            p = jnp.exp2(sc * (SCALE * LOG2E))
            if masked:
                row = lax.broadcasted_iota(jnp.int32, p.shape, 0)
                col = lax.broadcasted_iota(jnp.int32, p.shape, 1)
                p = jnp.where((col > row) & (col // blk == row // blk), 0.0, p)
            ds = (p * dp).astype(BF)
            pbig[h * chip:(h + 1) * chip, :] = p.astype(BF)
            dsbig[h * chip:(h + 1) * chip, :] = ds
        for h in range(RATIO):
            dqacc[h] += jnp.dot(dsbig[h * chip:(h + 1) * chip, :], key, preferred_element_type=F32)
        pbuf[d, e, 0] = (jnp.dot(qt[...], dsbig[...], preferred_element_type=F32) * SCALE).astype(BF)
        pbuf[d, e, 1] = jnp.dot(dot_[...], pbig[...], preferred_element_type=F32).astype(BF)

    def relay(e, w):
        return rcopy(pbuf.at[2, e, w], ra.at[e, w], ras.at[e, w], rar.at[e, w], (xm, xp)[w])

    def near(d, e, w):
        i = (d - 1) // 2
        return rcopy(pbuf.at[d, e, w], r1.at[i, e, w], r1s.at[i, e, w], r1r.at[i, e, w], xm if d == 1 else xp)

    def r2_copy(e, w):
        return rcopy(s2.at[e, w], r2.at[e, w], r2s.at[e, w], r2r.at[e, w], (dev(x, up(y, -e), c), z))

    def relays(e):
        relay(e, 0).start()
        relay(e, 1).start()

    def plain(d, e):
        near(d, e, 1 if d == 1 else 0).start()

    def join(d, e):
        w = 0 if d == 1 else 1
        with jax.named_scope('ra'):
            relay(e, w).wait_recv()
        pbuf[d, e, w] = (pbuf[d, e, w].astype(F32) + ra[e, w].astype(F32)).astype(BF)
        near(d, e, w).start()

    def sum_x(e, w):
        with jax.named_scope('r1'):
            near(1, e, w).wait_recv()
            near(3, e, w).wait_recv()
        return pbuf[0, e, w].astype(F32) + r1[0, e, w].astype(F32) + r1[1, e, w].astype(F32)

    def combine(e):
        for w in range(2):
            s2[e, w] = sum_x(e, w).astype(BF)

    def got_x():
        ax(1, at(1, 0)).wait_recv()
        ay(1, 1, at(1, 0)).start()
        fx(0, at(1, 0)).start()
        ax(3, at(3, 0)).wait_recv()
        ay(3, 3, at(3, 0)).start()
        fx(1, at(3, 0)).start()
        ay(0, 1, at(0, 1)).wait_recv()

    def got_far_x():
        fx(0, at(2, 0)).wait_recv()
        fx(1, at(2, 0)).wait_recv()
        ay(2, 1, at(2, 0)).start()
        ay(2, 3, at(2, 0)).start()
        ay(3, 1, at(3, 0)).start()
        ay(1, 3, at(1, 0)).start()

    def got_y(d, e):
        ay(d, e, at(d, e)).wait_recv()

    def far_k(d):
        fy(d, 0, at(d, 1)).start()

    def far_v(d):
        fy(d, 1, at(d, 3)).start()

    def got_far_y(d):
        fy(d, 0, at(d, 2)).wait_recv()
        fy(d, 1, at(d, 2)).wait_recv()

    def r2_send(e):
        r2_copy(e, 0).start()
        r2_copy(e, 1).start()

    events = {
        1: lambda: got_x(),
        2: lambda: got_y(0, 3),
        3: lambda: got_far_x(),
        4: lambda: (got_y(1, 1), relays(0)),
        5: lambda: (got_y(3, 3), plain(1, 1)),
        6: lambda: (got_y(2, 1), far_k(2), plain(3, 3)),
        7: lambda: (got_y(2, 3), far_v(2), relays(1)),
        8: lambda: (got_y(3, 1), far_k(0), far_v(0), relays(3)),
        9: lambda: (got_y(1, 3), plain(3, 1), far_k(1), far_v(1), far_k(3), far_v(3)),
        10: lambda: (got_far_y(2), plain(1, 3), join(1, 1), join(3, 1)),
        11: lambda: (got_far_y(0), relays(2), join(3, 3), join(1, 3)),
        12: lambda: got_far_y(1),
        13: lambda: (got_far_y(3), combine(1)),
        14: lambda: (plain(3, 2), join(1, 2), plain(1, 2), join(3, 2), r2_send(1), combine(3)),
        15: lambda: (plain(1, 0), join(1, 0), r2_send(3)),
    }

    with jax.named_scope('comp0'):
        compute(0, 0, True)

    def step(t, carry):
        for g in range(4):
            @pl.when(t // 4 == g)
            def _():
                for k in range(max(1, 4 * g), 4 * g + 4):
                    @pl.when(t == k)
                    def _():
                        with jax.named_scope('ev%d' % k):
                            events[k]()
        with jax.named_scope('comp'):
            code = pick(t, [d + 4 * e for d, e in ORDER])
            compute(lax.rem(code, 4), lax.div(code, 4), False)
        return carry

    lax.fori_loop(1, 16, step, 0)
    plain(3, 0)
    join(3, 0)

    orow = pl.multiple_of((1 - c) * rows, rows)
    mrow = pl.multiple_of(c * rows, rows)
    with jax.named_scope('dq'):
        for h in range(RATIO):
            dqs[:, h * HEAD_SIZE:(h + 1) * HEAD_SIZE] = (dqacc[h, pl.ds(orow, rows), :] * SCALE).astype(BF)
        for h in range(RATIO):
            cols = pl.ds(pl.multiple_of(mine + h * HEAD_SIZE, HEAD_SIZE), HEAD_SIZE)
            dq_ref[:, cols] = (dqacc[h, pl.ds(mrow, rows), :] * SCALE).astype(BF)
    for w in range(2):
        s2[2, w] = sum_x(2, w).astype(BF)
        r2_copy(2, w).start()
    dq_copy = rcopy(dqs, dq_ref.at[:, pl.ds(mine, half)], dqss.at[0], dqsr.at[0], sib)
    dq_copy.start()

    def s4_copy(r, w):
        cc, zz = member(r)
        off = pl.multiple_of(cc * rows + zz * piece, piece)
        dst = (dk_ref, dv_ref)[w].at[:, pl.ds(own_g, HEAD_SIZE)]
        return rcopy(fin.at[w, pl.ds(off, piece), :], dst, s4s.at[r, w], s4r.at[r, w], (dev(x, y, cc), zz))

    for w in range(2):
        tot = sum_x(0, w)
        for e in (1, 3, 2):
            with jax.named_scope('r2w'):
                r2_copy(e, w).wait_recv()
            tot = tot + r2[e, w].astype(F32)
        fin[w] = tot.T.astype(BF)
        for r in range(1, nm):
            s4_copy(r, w).start()
    dk_ref[:, pl.ds(own_g, HEAD_SIZE)] = fin[0, pl.ds(own_off, piece), :]
    dv_ref[:, pl.ds(own_g, HEAD_SIZE)] = fin[1, pl.ds(own_off, piece), :]

    def s4_wait(r, w):
        m = (me - r + nm) % nm
        cc, zz = m // nz, m % nz
        g = pl.multiple_of((2 * zz + cc) * HEAD_SIZE, HEAD_SIZE)
        dst = (dk_ref, dv_ref)[w].at[:, pl.ds(g, HEAD_SIZE)]
        rcopy(fin.at[w, pl.ds(0, piece), :], dst, s4s.at[r, w], s4r.at[r, w], sib).wait_recv()

    with jax.named_scope('s4w'):
        for r in range(1, nm):
            for w in range(2):
                s4_wait(r, w)
    rcopy(dqs, dq_ref.at[:, pl.ds(other, half)], dqss.at[0], dqsr.at[0], sib).wait_recv()

    for r in range(1, nm):
        for w in range(2):
            s0_copy(r, w).wait_send()
            s4_copy(r, w).wait_send()
    for cp in sib_copies:
        cp.wait_send()
    dq_copy.wait_send()
    for d in (1, 3):
        ax(d, at(0, 0)).wait_send()
    for w in range(2):
        fx(w, at(0, 0)).wait_send()
        for e in (1, 2, 3):
            r2_copy(e, w).wait_send()
        for e in range(4):
            relay(e, w).wait_send()
            near(1, e, w).wait_send()
            near(3, e, w).wait_send()
        for d in range(4):
            fy(d, w, at(0, 0)).wait_send()
    for d in range(4):
        ay(d, 1, at(0, 0)).wait_send()
        ay(d, 3, at(0, 0)).wait_send()


def fused(nz, queries, keys, values, outputs, out_grad, log_norm, block_order):
    rows, piece = queries.shape[0], keys.shape[0]
    chip = 2 * rows
    half = RATIO * HEAD_SIZE
    nm = 2 * nz
    dma = pltpu.SemaphoreType.DMA
    vm = pl.BlockSpec(memory_space=pltpu.VMEM)
    hbm = pl.BlockSpec(memory_space=pltpu.HBM)
    return pl.pallas_call(
        functools.partial(kernel, nz),
        out_shape=(
            jax.ShapeDtypeStruct(queries.shape, BF),
            jax.ShapeDtypeStruct(keys.shape, BF),
            jax.ShapeDtypeStruct(values.shape, BF),
        ),
        in_specs=[hbm] * 7,
        out_specs=(vm, vm, vm),
        scratch_shapes=[
            pltpu.VMEM(queries.shape, BF),
            pltpu.VMEM(keys.shape, BF),
            pltpu.VMEM(values.shape, BF),
            pltpu.VMEM(outputs.shape, BF),
            pltpu.VMEM(out_grad.shape, BF),
            pltpu.VMEM(log_norm.shape, F32),
            pltpu.SMEM(block_order.shape, jnp.int32),
            pltpu.VMEM((4, 4, 2, chip, HEAD_SIZE), BF),
            pltpu.VMEM((rows, half), BF),
            pltpu.VMEM((rows, half), BF),
            pltpu.VMEM((rows, half), BF),
            pltpu.VMEM(log_norm.shape, F32),
            pltpu.VMEM((HEAD_SIZE, rows), F32),
            pltpu.VMEM((rows, HEAD_SIZE), F32),
            pltpu.VMEM((RATIO, chip, 2 * HEAD_SIZE), BF),
            pltpu.VMEM((RATIO, chip, 2 * HEAD_SIZE), BF),
            pltpu.VMEM((HEAD_SIZE, RATIO * chip), BF),
            pltpu.VMEM((HEAD_SIZE, RATIO * chip), BF),
            pltpu.VMEM((chip, HEAD_SIZE), BF),
            pltpu.VMEM((RATIO * chip, chip), BF),
            pltpu.VMEM((RATIO * chip, chip), BF),
            pltpu.VMEM((RATIO, chip, HEAD_SIZE), F32),
            pltpu.VMEM((4, 4, 2, HEAD_SIZE, chip), BF),
            pltpu.VMEM((2, 4, 2, HEAD_SIZE, chip), BF),
            pltpu.VMEM((4, 2, HEAD_SIZE, chip), BF),
            pltpu.VMEM((4, 2, HEAD_SIZE, chip), BF),
            pltpu.VMEM((4, 2, HEAD_SIZE, chip), BF),
            pltpu.VMEM((2, chip, HEAD_SIZE), BF),
            pltpu.VMEM((rows, half), BF),
            dma((7,)),
            dma((nm, 2)), dma((nm, 2)), dma((4,)), dma((4,)),
            dma((4,)), dma((4,)), dma((4, 4)), dma((4, 4)),
            dma((2,)), dma((2,)), dma((4, 2)), dma((4, 2)),
            dma((2, 4, 2)), dma((2, 4, 2)), dma((4, 2)), dma((4, 2)),
            dma((4, 2)), dma((4, 2)), dma((nm, 2)), dma((nm, 2)), dma((1,)), dma((1,)),
        ],
        compiler_params=pltpu.CompilerParams(
            collective_id=0, has_side_effects=True, vmem_limit_bytes=40 * 1024 * 1024),
    )(*(pltpu.with_memory_space_constraint(a, pltpu.HBM) for a in (
        queries, keys, values, outputs, out_grad, log_norm, block_order)))


def solution(mesh):
    in_specs = (
        P("seq", "head"),
        P(("seq", "head"), None),
        P(("seq", "head"), None),
        P("seq", "head"),
        P("seq", "head"),
        P("head", "seq"),
        P(),
    )
    out_specs = (P("seq", "head"), P(("seq", "head"), None), P(("seq", "head"), None))
    return jax.shard_map(
        functools.partial(fused, mesh.shape["head"]), mesh=mesh,
        in_specs=in_specs, out_specs=out_specs, check_vma=False)
```
